32 devices in a mesh: ka: 8 (over y, x, core), ga: 4 (over z).
Axes of the slice: x: 2, y: 2, z: 4, core: 2. Of those that a mesh axis runs over, the one named last changes fastest.
Arguments:
- pair_densities: float32 [8192, 8192], P('ka', 'ga'), may hold values from -0.0625 to 0.0625
- energies: float32 [8192], P('ka'), may hold values from -2 to 2
- coulomb: float32 [8192], P('ga'), may hold values from 0.2 to 2
- start: float32 [8192, 128], P('ka'), may hold values from -6 to 6
Outputs:
- alphas: float32 [4, 128], replicated
- betas: float32 [4, 128], replicated
- lanczos_vector: float32 [8192, 128], P('ka')
The draws below stay inside these ranges and needn't reach their ends.
All inputs are finite; a program needn't handle non-finite values.
Results may differ from the reference program's by a relative error of at most 0.00013.
Values sent between devices are 32-bit elements; how exact they have to be, the bound alone decides.
No kernel may reach another device: no remote copies, remote signals or barrier semaphores. Data moves between devices by JAX's collectives and lax.ppermute only.
A program may use at most 64 MiB of HBM per device.

```python
import math
import jax
import jax.numpy as jnp
from jax import lax

G = 8192
NV = 128
ITERS = 4
ROWS = 8192


def levels(stream_key, dims, pieces, smallest, high):
    factor_of = 1.0
    for dim, blocks in pieces:
        heights = jax.random.uniform(jax.random.fold_in(jax.random.fold_in(stream_key, 6), dim), (blocks,), jnp.float32, smallest / len(pieces), high / len(pieces))
        factor_of = factor_of * jnp.repeat(jnp.exp(heights), dims[dim] // blocks).reshape((-1,) + (1,) * (len(dims) - 1 - dim))
    return factor_of


def scatter_about(rng, dims, deviation, most, split=(), dtype=jnp.bfloat16):
    entries = deviation * jax.random.normal(rng, dims, jnp.float32)
    if split:
        entries = entries * levels(rng, dims, split, -0.22, 0.18)
    return jnp.clip(entries, -most, most).astype(dtype)


def setup_inputs(seed: int = 0) -> dict:
    key_list = jax.random.split(jax.random.key(seed), 5)
    pair_densities = scatter_about(key_list[0], (ROWS, G), ROWS ** -0.5, 0.0625, ((0, 8), (1, 4)), jnp.float32)
    energies = jnp.clip(jax.random.uniform(key_list[1], (ROWS,), jnp.float32, -2.0, 2.0) * levels(key_list[1], (ROWS,), ((0, 8),), -0.4, 0.0), -2.0, 2.0)
    coulomb = jnp.clip(jnp.exp(math.log(2.0) - 2.3025851 * jax.random.uniform(key_list[2], (G,), jnp.float32) ** levels(key_list[2], (G,), ((0, 4),), -0.2, 0.2)), 0.2, 2.0)
    start = scatter_about(key_list[3], (ROWS, NV), 1.0, 6.0, ((0, 8),), jnp.float32)
    return {"pair_densities": pair_densities, "energies": energies, "coulomb": coulomb, "start": start}


EPSILON = 1e-06

def reference(pair_densities, energies, coulomb, start):
    precise = lax.Precision.HIGHEST

    def apply_ham(vector):
        projected = jnp.dot(pair_densities.T, vector, precision=precise, preferred_element_type=jnp.float32)
        weighted = coulomb[:, None] * projected
        mixed = jnp.dot(pair_densities, weighted, precision=precise, preferred_element_type=jnp.float32)
        return energies[:, None] * vector + mixed
    vector = start / jnp.sqrt(lax.optimization_barrier(jnp.sum(start * start, axis=0)) + EPSILON)
    previous = jnp.zeros_like(vector)
    beta_now = jnp.zeros((vector.shape[1],), jnp.float32)
    alpha_rows = []
    beta_rows = []
    for step in range(ITERS):
        image = apply_ham(vector)
        alpha_now = lax.optimization_barrier(jnp.sum(vector * image, axis=0))
        remainder = image - alpha_now * vector - beta_now * previous
        beta_new = jnp.sqrt(lax.optimization_barrier(jnp.sum(remainder * remainder, axis=0)) + EPSILON)
        previous = vector
        vector = remainder / beta_new
        beta_now = beta_new
        alpha_rows.append(alpha_now)
        beta_rows.append(beta_new)
    return (jnp.stack(alpha_rows), jnp.stack(beta_rows), vector)
```

```python
import functools

import jax
import jax.numpy as jnp
from jax import lax
from jax.experimental import pallas as pl
from jax.experimental.pallas import tpu as pltpu
from jax.sharding import PartitionSpec as P

ITERS = 4
EPSILON = 1e-06
LANES = 128
PACK = 1
SCALARS = 8


VMEM = pl.BlockSpec(memory_space=pltpu.VMEM)
SMEM = pl.BlockSpec(memory_space=pltpu.SMEM)


def call(body, outs, scratch, flops, *args, scalars=0):
    specs = [SMEM] * scalars + [VMEM] * (len(args) - scalars)
    return pl.pallas_call(
        body,
        out_shape=[jax.ShapeDtypeStruct(shape, dtype) for shape, dtype in outs],
        in_specs=specs,
        out_specs=[VMEM] * len(outs),
        scratch_shapes=[pltpu.VMEM(shape, dtype) for shape, dtype in scratch],
        cost_estimate=pl.CostEstimate(flops=flops, bytes_accessed=0, transcendentals=0),
        compiler_params=pltpu.CompilerParams(vmem_limit_bytes=40 * 1024 * 1024),
    )(*args)


def split_matrix(m_ref, hi_ref, lo_ref, t_hi_ref, t_lo_ref):
    rows, cols = m_ref.shape
    tile = 256

    def row_step(i, _):
        at = pl.ds(pl.multiple_of(i * tile, tile), tile)

        def col_step(j, _):
            to = pl.ds(pl.multiple_of(j * tile, tile), tile)
            x = m_ref[at, to]
            hi = x.astype(jnp.bfloat16)
            lo = x - hi.astype(jnp.float32)
            hi_ref[at, to] = hi
            lo_ref[at, to] = lo.astype(jnp.bfloat16)
            x_t = x.T
            hi_t = x_t.astype(jnp.bfloat16)
            t_hi_ref[to, at] = hi_t
            t_lo_ref[to, at] = (x_t - hi_t.astype(jnp.float32)).astype(jnp.bfloat16)
            return 0

        return lax.fori_loop(0, cols // tile, col_step, 0)

    lax.fori_loop(0, rows // tile, row_step, 0)


def left_lanes(shape):
    return lax.broadcasted_iota(jnp.int32, shape, 1) < LANES // 2


def lane_sum(row):
    return row if PACK == 1 else row + pltpu.roll(row, LANES // 2, 1)


def fill_rhs(rhs_ref, at, size, half, x):
    hi = x.astype(jnp.bfloat16).astype(jnp.float32)
    lo = x - hi
    if PACK == 1:
        rhs_ref[pl.ds(at, size), :LANES] = hi.astype(jnp.bfloat16)
        rhs_ref[pl.ds(at, size), LANES:] = lo.astype(jnp.bfloat16)
        return
    left = left_lanes(x.shape)
    turn = LANES // 2
    top = jnp.where(left, hi, pltpu.roll(lo, turn, 1))
    bottom = jnp.where(left, pltpu.roll(hi, turn, 1), lo)
    rhs_ref[pl.ds(at, size), :] = top.astype(jnp.bfloat16)
    rhs_ref[pl.ds(at + half, size), :] = bottom.astype(jnp.bfloat16)


def dot2(hi_ref, lo_ref, rhs_ref, at, size):
    rhs = rhs_ref[...]
    rows = pl.ds(at, size)
    return jnp.dot(hi_ref[rows, :], rhs, preferred_element_type=jnp.float32) + jnp.dot(
        lo_ref[rows, :], rhs, preferred_element_type=jnp.float32
    )


def product_rows(hi_ref, lo_ref, rhs_ref, at, size, half):
    if PACK == 1:
        both = dot2(hi_ref, lo_ref, rhs_ref, at, size)
        return both[:, :LANES] + both[:, LANES:]
    turn = LANES // 2
    top = dot2(hi_ref, lo_ref, rhs_ref, at, size)
    bottom = dot2(hi_ref, lo_ref, rhs_ref, at + half, size)
    top = top + pltpu.roll(top, turn, 1)
    bottom = bottom + pltpu.roll(bottom, turn, 1)
    return jnp.where(left_lanes(top.shape), top, bottom)


def product(hi_ref, lo_ref, rhs_ref, own, send_ref, keep_ref):
    half = hi_ref.shape[0] // 2
    part = hi_ref.shape[0] // PACK // 2
    tile = min(part, 512 // PACK)
    for owner, ref in ((1 - own, send_ref), (own, keep_ref)):

        def step(i, _):
            to = pl.multiple_of(i * tile, tile)
            at = pl.multiple_of(owner * part + i * tile, tile)
            ref[pl.ds(to, tile), :] = product_rows(hi_ref, lo_ref, rhs_ref, at, tile, half)
            return 0

        lax.fori_loop(0, part // tile, step, 0)


def put_scalars(refs, rows):
    at = refs[0].shape[0] - SCALARS
    block = jnp.concatenate(rows + [jnp.zeros((SCALARS - len(rows), LANES), jnp.float32)], axis=0)
    for ref in refs:
        ref[at:, :] = block


def project(first, own_ref, t_hi_ref, t_lo_ref, energy_ref, *refs):
    if first:
        r_ref, send_ref, keep_ref, rhs_ref = refs
        r = r_ref[...]
    else:
        fixed_ref, own_half_ref, other_half_ref, r_ref, v_ref = refs[:5]
        send_ref, keep_ref, next_ref, unit_ref, alpha_ref, rhs_ref = refs[5:]
        r = advance(own_ref[1], energy_ref, fixed_ref, own_half_ref, other_half_ref, r_ref, v_ref, unit_ref, alpha_ref)
        next_ref[...] = r
    energy = energy_ref[...]
    square = r * r
    square_row = lane_sum(jnp.sum(square, axis=0, keepdims=True))
    energy_row = lane_sum(jnp.sum(square * energy, axis=0, keepdims=True))
    size = r.shape[0]
    fill_rhs(rhs_ref, 0, size, size, r)
    product(t_hi_ref, t_lo_ref, rhs_ref, own_ref[0], send_ref, keep_ref)
    put_scalars([send_ref, keep_ref], [square_row, energy_row])


def advance(own, energy_ref, fixed_ref, own_half_ref, other_half_ref, r_ref, v_ref, unit_ref, alpha_ref):
    part = other_half_ref.shape[0]
    beta = fixed_ref[0:1, :]
    energy_sum = fixed_ref[1:2, :]
    alpha = energy_sum + own_half_ref[part : part + 1, :]
    alpha_ref[...] = alpha
    inverse = 1.0 / beta
    first_half = jnp.where(own == 0, own_half_ref[:part, :], other_half_ref[...])
    second_half = jnp.where(own == 0, other_half_ref[...], own_half_ref[:part, :])
    pieces = []
    for index, mixed in enumerate((first_half, second_half)):
        at = slice(index * part, (index + 1) * part)
        unit = r_ref[at, :] * inverse
        unit_ref[at, :] = unit
        pieces.append(
            energy_ref[at, :] * unit + mixed - alpha * unit - beta * v_ref[at, :]
        )
    return jnp.concatenate(pieces, axis=0)


def exchange(own_ref, hi_ref, lo_ref, coulomb_ref, own_half_ref, other_half_ref, send_ref, keep_ref, fixed_ref, rhs_ref):
    part = coulomb_ref.shape[0] // 2
    core = own_ref[0]
    sums = jnp.where(core == 0, own_half_ref[part:, :], other_half_ref[part:, :])
    beta = jnp.sqrt(sums[0:1, :] + EPSILON)
    inverse = 1.0 / beta
    energy_sum = sums[1:2, :] * inverse * inverse
    fixed_ref[...] = jnp.concatenate([beta, energy_sum, jnp.zeros((SCALARS - 2, LANES), jnp.float32)], axis=0)
    tile = min(part, 256)
    total = jnp.zeros((1, LANES), jnp.float32)
    for owner, ref in ((core, own_half_ref), (1 - core, other_half_ref)):

        def step(i, total):
            at = pl.multiple_of(i * tile, tile)
            to = pl.multiple_of(owner * part + i * tile, tile)
            projected = ref[pl.ds(at, tile), :] * inverse
            weighted = coulomb_ref[pl.ds(to, tile), :] * projected
            fill_rhs(rhs_ref, to, tile, 2 * part, weighted)
            return total + jnp.sum(projected * weighted, axis=0, keepdims=True)

        if ref is own_half_ref:
            own_total = lax.fori_loop(0, part // tile, step, total)
        else:
            other_total = lax.fori_loop(0, part // tile, step, total)
    curvature = lane_sum(own_total + other_total)
    product(hi_ref, lo_ref, rhs_ref, own_ref[1], send_ref, keep_ref)
    put_scalars([send_ref, keep_ref], [curvature])


def finish(own_ref, energy_ref, fixed_ref, own_half_ref, other_half_ref, r_ref, v_ref, next_ref, square_ref, alpha_ref, unit_ref):
    r = advance(own_ref[1], energy_ref, fixed_ref, own_half_ref, other_half_ref, r_ref, v_ref, unit_ref, alpha_ref)
    next_ref[...] = r
    square = lane_sum(jnp.sum(r * r, axis=0, keepdims=True))
    square_ref[...] = jnp.concatenate([square, jnp.zeros((SCALARS - 1, LANES), jnp.float32)], axis=0)


def swaps(size, bit):
    return [(i, i ^ bit) for i in range(size)]


def crossed_swaps(size):
    bits = [1 << b for b in range(1, size.bit_length() - 1)]
    turned = bits[::-1]
    return [
        [(i, i ^ (turned[n] if i & 1 else bits[n])) for i in range(size)] for n in range(len(bits))
    ]


def bits_from(size, low):
    return [1 << b for b in range(low, size.bit_length() - 1)]


def per_device(ka, ga, pair_densities, energies, coulomb, start):
    rows, cols = pair_densities.shape
    columns = start.shape[1]
    f32, b16 = jnp.float32, jnp.bfloat16
    r_rows, g_rows = rows // PACK, cols // PACK
    r_part, g_part = r_rows // 2, g_rows // 2
    own = jnp.stack([lax.axis_index("ka") & 1, lax.axis_index("ga") & 1]).astype(jnp.int32)
    hi, lo, t_hi, t_lo = call(
        split_matrix,
        [((rows, cols), b16)] * 2 + [((cols, rows), b16)] * 2,
        [],
        2**31,
        pair_densities,
    )
    energy = jnp.broadcast_to(energies[:, None], (rows, LANES))
    weights = jnp.broadcast_to(coulomb[:, None], (cols, LANES))
    wide = 2 * LANES // PACK
    flops = 4 * rows * cols * LANES
    sums = (SCALARS, LANES)
    line = (1, LANES)

    alphas, betas = [], []
    r = start
    v = jnp.zeros_like(r)
    fixed = own_half = other_half = None
    for step in range(ITERS):
        shapes = [((g_part + SCALARS, LANES), f32)] * 2
        rhs = [((rows, wide), b16)]
        if step == 0:
            send, keep = call(
                functools.partial(project, True), shapes, rhs, flops, own, t_hi, t_lo, energy, r, scalars=1
            )
        else:
            send, keep, r, v, alpha = call(
                functools.partial(project, False),
                shapes + [((r_rows, LANES), f32)] * 2 + [(line, f32)],
                rhs,
                flops,
                own,
                t_hi,
                t_lo,
                energy,
                fixed,
                own_half,
                other_half,
                r,
                v,
                scalars=1,
            )
            alphas.append(alpha)
        held = keep + lax.ppermute(send, "ka", swaps(ka, 1))
        for pairs in crossed_swaps(ka):
            held = held + lax.ppermute(held, "ka", pairs)
        other = lax.ppermute(held, "ka", swaps(ka, 1))
        send, keep, fixed = call(
            exchange,
            [((r_part + SCALARS, LANES), f32)] * 2 + [(sums, f32)],
            [((cols, wide), b16)],
            flops,
            own,
            hi,
            lo,
            weights,
            held,
            other,
            scalars=1,
        )
        if step > 0:
            betas.append(fixed[0:1])
        own_half = keep + lax.ppermute(send, "ga", swaps(ga, 1))
        for bit in bits_from(ga, 1):
            own_half = own_half + lax.ppermute(own_half, "ga", swaps(ga, bit))
        other_half = lax.ppermute(own_half[:r_part], "ga", swaps(ga, 1))
    r, square, alpha, _ = call(
        finish,
        [((r_rows, LANES), f32), (sums, f32), (line, f32), ((r_rows, LANES), f32)],
        [],
        2**20,
        own,
        energy,
        fixed,
        own_half,
        other_half,
        r,
        v,
        scalars=1,
    )
    alphas.append(alpha)
    for bit in bits_from(ka, 0):
        square = square + lax.ppermute(square, "ka", swaps(ka, bit))
    beta = jnp.sqrt(square[0:1] + EPSILON)
    betas.append(beta)
    return (jnp.concatenate(alphas, axis=0), jnp.concatenate(betas, axis=0), r / beta)


def solution(mesh):
    placed = (P("ka", "ga"), P("ka"), P("ga"), P("ka", None))
    return jax.shard_map(
        functools.partial(per_device, mesh.shape["ka"], mesh.shape["ga"]),
        mesh=mesh,
        in_specs=placed,
        out_specs=(P(), P(), P("ka", None)),
        check_vma=False,
    )
```

```python
import functools

import jax
import jax.numpy as jnp
from jax import lax
from jax.experimental import pallas as pl
from jax.experimental.pallas import tpu as pltpu
from jax.sharding import PartitionSpec as P

ITERS = 4
EPSILON = 1e-06
LANES = 128
PACK = 1
ROWS = 8


VMEM = pl.BlockSpec(memory_space=pltpu.VMEM)
SMEM = pl.BlockSpec(memory_space=pltpu.SMEM)


def call(body, outs, scratch, flops, *args, scalars=0):
    specs = [SMEM] * scalars + [VMEM] * (len(args) - scalars)
    return pl.pallas_call(
        body,
        out_shape=[jax.ShapeDtypeStruct(shape, dtype) for shape, dtype in outs],
        in_specs=specs,
        out_specs=[VMEM] * len(outs),
        scratch_shapes=[pltpu.VMEM(shape, dtype) for shape, dtype in scratch],
        cost_estimate=pl.CostEstimate(flops=flops, bytes_accessed=0, transcendentals=0),
        compiler_params=pltpu.CompilerParams(vmem_limit_bytes=8 * 1024 * 1024),
    )(*args)


def split_matrix(own_ref, m_ref, hi_ref, lo_ref, t_hi_ref, t_lo_ref, held_ref, arrived):
    rows, cols = m_ref.shape
    tile = min(rows, 128)
    wide = min(cols, 512)
    copies = []
    for i in range(rows // tile):
        at = pl.ds(i * tile, tile)
        copies.append(pltpu.make_async_copy(m_ref.at[at, :], held_ref.at[at, :], arrived.at[i]))
        copies[-1].start()
    for i in range(rows // tile):
        at = pl.ds(i * tile, tile)
        copies[i].wait()

        def step(j, _):
            to = pl.ds(pl.multiple_of(j * wide, wide), wide)
            x = held_ref[at, to]
            hi = x.astype(jnp.bfloat16)
            lo = x - hi.astype(jnp.float32)
            hi_ref[at, to] = hi
            lo_ref[at, to] = lo.astype(jnp.bfloat16)
            t_hi_ref[to, at] = x.T.astype(jnp.bfloat16)
            t_lo_ref[to, at] = lo.T.astype(jnp.bfloat16)
            return 0

        lax.fori_loop(0, cols // wide, step, 0)


def left_lanes(shape):
    return lax.broadcasted_iota(jnp.int32, shape, 1) < LANES // 2


def lane_sum(row):
    return row if PACK == 1 else row + pltpu.roll(row, LANES // 2, 1)


def fill_rhs(rhs_ref, at, size, half, x):
    hi = x.astype(jnp.bfloat16).astype(jnp.float32)
    lo = x - hi
    if PACK == 1:
        rhs_ref[pl.ds(at, size), :LANES] = hi.astype(jnp.bfloat16)
        rhs_ref[pl.ds(at, size), LANES:] = lo.astype(jnp.bfloat16)
        return
    left = left_lanes(x.shape)
    turn = LANES // 2
    top = jnp.where(left, hi, pltpu.roll(lo, turn, 1))
    bottom = jnp.where(left, pltpu.roll(hi, turn, 1), lo)
    rhs_ref[pl.ds(at, size), :] = top.astype(jnp.bfloat16)
    rhs_ref[pl.ds(at + half, size), :] = bottom.astype(jnp.bfloat16)


def dot2(hi_ref, lo_ref, rhs_ref, at, size):
    rhs = rhs_ref[...]
    rows = pl.ds(at, size)
    return jnp.dot(hi_ref[rows, :], rhs, preferred_element_type=jnp.float32) + jnp.dot(
        lo_ref[rows, :], rhs, preferred_element_type=jnp.float32
    )


def product_rows(hi_ref, lo_ref, rhs_ref, at, size, half):
    if PACK == 1:
        both = dot2(hi_ref, lo_ref, rhs_ref, at, size)
        return both[:, :LANES] + both[:, LANES:]
    turn = LANES // 2
    top = dot2(hi_ref, lo_ref, rhs_ref, at, size)
    bottom = dot2(hi_ref, lo_ref, rhs_ref, at + half, size)
    top = top + pltpu.roll(top, turn, 1)
    bottom = bottom + pltpu.roll(bottom, turn, 1)
    return jnp.where(left_lanes(top.shape), top, bottom)


def product(hi_ref, lo_ref, rhs_ref, own, send_ref, keep_ref):
    half = hi_ref.shape[0] // 2
    part = hi_ref.shape[0] // PACK // 2
    tile = min(part, 512 // PACK)
    for owner, ref in ((1 - own, send_ref), (own, keep_ref)):

        def step(i, _):
            to = pl.multiple_of(i * tile, tile)
            at = pl.multiple_of(owner * part + i * tile, tile)
            ref[pl.ds(to, tile), :] = product_rows(hi_ref, lo_ref, rhs_ref, at, tile, half)
            return 0

        lax.fori_loop(0, part // tile, step, 0)


def block_of(rows, size=ROWS):
    return jnp.concatenate(rows + [jnp.zeros((size - len(rows), LANES), jnp.float32)], axis=0)


def project(first, own_ref, t_hi_ref, t_lo_ref, energy_ref, *refs):
    if first:
        r_ref, send_ref, keep_ref, rhs_ref = refs
        r = r_ref[...]
    else:
        fixed_ref, own_half_ref, other_half_ref, r_ref, v_ref = refs[:5]
        send_ref, keep_ref, next_ref, unit_ref, alpha_ref, rhs_ref = refs[5:]
        r = advance(own_ref[1], energy_ref, fixed_ref, own_half_ref, other_half_ref, r_ref, v_ref, unit_ref, alpha_ref)
        next_ref[...] = r
    energy = energy_ref[...]
    square = r * r
    square_row = lane_sum(jnp.sum(square, axis=0, keepdims=True))
    energy_row = lane_sum(jnp.sum(square * energy, axis=0, keepdims=True))
    size = r.shape[0]
    fill_rhs(rhs_ref, 0, size, size, r)
    product(t_hi_ref, t_lo_ref, rhs_ref, own_ref[0], send_ref, keep_ref)
    for ref in (send_ref, keep_ref):
        ref[ref.shape[0] - ROWS :, :] = block_of([square_row, energy_row])


def advance(own, energy_ref, fixed_ref, own_half_ref, other_half_ref, r_ref, v_ref, unit_ref, alpha_ref):
    part = other_half_ref.shape[0]
    beta = fixed_ref[0:1, :]
    energy_sum = fixed_ref[1:2, :]
    alpha = energy_sum + jnp.sum(own_half_ref[part:, :], axis=0, keepdims=True)
    alpha_ref[...] = alpha
    inverse = 1.0 / beta
    first_half = jnp.where(own == 0, own_half_ref[:part, :], other_half_ref[...])
    second_half = jnp.where(own == 0, other_half_ref[...], own_half_ref[:part, :])
    pieces = []
    for index, mixed in enumerate((first_half, second_half)):
        at = slice(index * part, (index + 1) * part)
        unit = r_ref[at, :] * inverse
        unit_ref[at, :] = unit
        pieces.append(
            energy_ref[at, :] * unit + mixed - alpha * unit - beta * v_ref[at, :]
        )
    return jnp.concatenate(pieces, axis=0)


def exchange(own_ref, hi_ref, lo_ref, coulomb_ref, own_half_ref, other_half_ref, send_ref, keep_ref, fixed_ref, rhs_ref):
    part = coulomb_ref.shape[0] // 2
    core = own_ref[0]
    sums = jnp.where(core == 0, own_half_ref[part:, :], other_half_ref[part:, :])
    beta = jnp.sqrt(sums[0:1, :] + EPSILON)
    inverse = 1.0 / beta
    energy_sum = sums[1:2, :] * inverse * inverse
    fixed_ref[...] = block_of([beta, energy_sum])
    tile = min(part, 256)
    total = jnp.zeros((1, LANES), jnp.float32)
    for owner, ref in ((core, own_half_ref), (1 - core, other_half_ref)):

        def step(i, total):
            at = pl.multiple_of(i * tile, tile)
            to = pl.multiple_of(owner * part + i * tile, tile)
            projected = ref[pl.ds(at, tile), :] * inverse
            weighted = coulomb_ref[pl.ds(to, tile), :] * projected
            fill_rhs(rhs_ref, to, tile, 2 * part, weighted)
            return total + jnp.sum(projected * weighted, axis=0, keepdims=True)

        if ref is own_half_ref:
            own_total = lax.fori_loop(0, part // tile, step, total)
        else:
            other_total = lax.fori_loop(0, part // tile, step, total)
    curvature = lane_sum(own_total + other_total)
    product(hi_ref, lo_ref, rhs_ref, own_ref[1], send_ref, keep_ref)
    for ref in (send_ref, keep_ref):
        at = hi_ref.shape[0] // PACK // 2
        row = lax.broadcasted_iota(jnp.int32, (ref.shape[0] - at, LANES), 0)
        ref[at:, :] = jnp.where(row == own_ref[2], curvature, 0.0)


def finish(own_ref, energy_ref, fixed_ref, own_half_ref, other_half_ref, r_ref, v_ref, next_ref, square_ref, alpha_ref, unit_ref):
    r = advance(own_ref[1], energy_ref, fixed_ref, own_half_ref, other_half_ref, r_ref, v_ref, unit_ref, alpha_ref)
    next_ref[...] = r
    square = lane_sum(jnp.sum(r * r, axis=0, keepdims=True))
    square_ref[...] = block_of([square])


def swaps(size, bit):
    return [(i, i ^ bit) for i in range(size)]


def bits_of(size):
    return [1 << b for b in range(size.bit_length() - 1)]


def crossed_swaps(size):
    bits = bits_of(size)[1:]
    turned = bits[::-1]
    return [
        [(i, i ^ (turned[n] if i & 1 else bits[n])) for i in range(size)] for n in range(len(bits))
    ]


def depth_swaps(ka, ga):
    bits = bits_of(ga)
    orders = [bits, bits[1:2] + bits[:1] + bits[2:]]
    return [
        [(a * ga + g, a * ga + (g ^ orders[a & 1][n])) for a in range(ka) for g in range(ga)]
        for n in range(len(bits))
    ]


def packed(x):
    return jnp.concatenate(jnp.split(x, PACK, axis=0), axis=1)


def unpacked(x):
    return jnp.concatenate(jnp.split(x, PACK, axis=1), axis=0)


def recursion(ka, ga, own, matrix, energy, weights, r):
    hi, lo, t_hi, t_lo = matrix
    rows, cols = hi.shape
    f32, b16 = jnp.float32, jnp.bfloat16
    r_rows, g_rows = rows // PACK, cols // PACK
    r_part, g_part = r_rows // 2, g_rows // 2
    z_rows = max(ROWS, ga)
    wide = 2 * LANES // PACK
    flops = 4 * rows * cols * LANES
    line = (1, LANES)
    both = ("ka", "ga")
    first_round, *rounds = depth_swaps(ka, ga)

    alphas, betas = [], []
    v = jnp.zeros_like(r)
    fixed = own_half = other_half = None
    for step in range(ITERS):
        shapes = [((g_part + ROWS, LANES), f32)] * 2
        rhs = [((rows, wide), b16)]
        if step == 0:
            send, keep = call(
                functools.partial(project, True), shapes, rhs, flops, own, t_hi, t_lo, energy, r, scalars=1
            )
        else:
            send, keep, r, v, alpha = call(
                functools.partial(project, False),
                shapes + [((r_rows, LANES), f32)] * 2 + [(line, f32)],
                rhs,
                flops,
                own,
                t_hi,
                t_lo,
                energy,
                fixed,
                own_half,
                other_half,
                r,
                v,
                scalars=1,
            )
            alphas.append(alpha)
        arrived = lax.ppermute(send, "ka", swaps(ka, 1))
        pieces = []
        for at in (slice(g_part // 2, None), slice(0, g_part // 2)):
            held = keep[at] + arrived[at]
            for pairs in crossed_swaps(ka):
                held = held + lax.ppermute(held, "ka", pairs)
            pieces.insert(0, (held, lax.ppermute(held, "ka", swaps(ka, 1))))
        held, other = (jnp.concatenate(part, axis=0) for part in zip(*pieces))
        send, keep, fixed = call(
            exchange,
            [((r_part + z_rows, LANES), f32)] * 2 + [((ROWS, LANES), f32)],
            [((cols, wide), b16)],
            flops,
            own,
            hi,
            lo,
            weights,
            held,
            other,
            scalars=1,
        )
        if step > 0:
            betas.append(fixed[0:1])
        pieces = []
        for at in (slice(r_part // 2, None), slice(0, r_part // 2)):
            own_half = keep[at] + lax.ppermute(send[at], both, first_round)
            for pairs in rounds:
                own_half = own_half + lax.ppermute(own_half, both, pairs)
            pieces.insert(0, (own_half, lax.ppermute(own_half[: r_part // 2], both, first_round)))
        own_half, other_half = (jnp.concatenate(part, axis=0) for part in zip(*pieces))
    r, square, alpha, _ = call(
        finish,
        [((r_rows, LANES), f32), ((ROWS, LANES), f32), (line, f32), ((r_rows, LANES), f32)],
        [],
        2**20,
        own,
        energy,
        fixed,
        own_half,
        other_half,
        r,
        v,
        scalars=1,
    )
    alphas.append(alpha)
    for bit in bits_of(ka):
        square = square + lax.ppermute(square, "ka", swaps(ka, bit))
    beta = jnp.sqrt(square[0:1] + EPSILON)
    betas.append(beta)
    width = LANES // PACK
    return (
        jnp.concatenate(alphas, axis=0)[:, :width],
        jnp.concatenate(betas, axis=0)[:, :width],
        unpacked(r / beta),
    )


def per_device(ka, ga, pair_densities, energies, coulomb, start):
    rows, cols = pair_densities.shape
    b16 = jnp.bfloat16
    core, depth = lax.axis_index("ka") & 1, lax.axis_index("ga")
    lead = jnp.where(core == 0, depth & 1, (depth >> 1) & 1)
    own = jnp.stack([core, lead, depth]).astype(jnp.int32)
    matrix = pl.pallas_call(
        split_matrix,
        out_shape=[jax.ShapeDtypeStruct((rows, cols), b16)] * 2
        + [jax.ShapeDtypeStruct((cols, rows), b16)] * 2,
        in_specs=[SMEM, pl.BlockSpec(memory_space=pltpu.HBM)],
        out_specs=[VMEM] * 4,
        scratch_shapes=[
            pltpu.VMEM((rows, cols), jnp.float32),
            pltpu.SemaphoreType.DMA((max(1, rows // 128),)),
        ],
        cost_estimate=pl.CostEstimate(flops=2**31, bytes_accessed=0, transcendentals=0),
        compiler_params=pltpu.CompilerParams(vmem_limit_bytes=34 * 1024 * 1024),
    )(own, pair_densities)
    width = LANES // PACK
    energy = packed(jnp.broadcast_to(energies[:, None], (rows, width)))
    weights = packed(jnp.broadcast_to(coulomb[:, None], (cols, width)))
    results = [
        recursion(ka, ga, own, matrix, energy, weights, packed(start[:, at : at + width]))
        for at in range(0, start.shape[1], width)
    ]
    return tuple(jnp.concatenate(parts, axis=1) for parts in zip(*results))


def solution(mesh):
    placed = (P("ka", "ga"), P("ka"), P("ga"), P("ka", None))
    return jax.shard_map(
        functools.partial(per_device, mesh.shape["ka"], mesh.shape["ga"]),
        mesh=mesh,
        in_specs=placed,
        out_specs=(P(), P(), P("ka", None)),
        check_vma=False,
    )
```

```python
import functools

import jax
import jax.numpy as jnp
from jax import lax
from jax.experimental import pallas as pl
from jax.experimental.pallas import tpu as pltpu
from jax.sharding import PartitionSpec as P

ITERS = 4
EPSILON = 1e-06
LANES = 128
TILE = 2048
KA_CUTS = (6,)
GA_CUTS = (8,)
ROWS = 8
MIB = 1024 * 1024


VMEM = pl.BlockSpec(memory_space=pltpu.VMEM)
SMEM = pl.BlockSpec(memory_space=pltpu.SMEM)
F32, B16 = jnp.float32, jnp.bfloat16

CORE, LEAD, DEPTH, CHIP = range(4)


def call(body, outs, flops, own, *args):
    return pl.pallas_call(
        body,
        out_shape=[jax.ShapeDtypeStruct(shape, dtype) for shape, dtype in outs],
        in_specs=[SMEM] + [VMEM] * len(args),
        out_specs=[VMEM] * len(outs),
        cost_estimate=pl.CostEstimate(flops=flops, bytes_accessed=0, transcendentals=0),
        compiler_params=pltpu.CompilerParams(vmem_limit_bytes=8 * MIB),
    )(own, *args)


def split_matrix(own_ref, m_ref, parts_ref, t_parts_ref, held_ref, arrived):
    rows, cols = m_ref.shape
    tile = min(rows // 2, 128)
    wide = min(cols // 2, 1024)
    copies = []
    for i in range(rows // tile):
        at = pl.ds(i * tile, tile)
        copies.append(pltpu.make_async_copy(m_ref.at[at, :], held_ref.at[at, :], arrived.at[i]))
        copies[-1].start()
    for i in range(rows // tile):
        at = pl.ds(i * tile, tile)
        side, place = divmod(i * tile, rows // 2)
        copies[i].wait()
        for half in range(2):

            def step(j, _):
                to = pl.multiple_of(j * wide, wide)
                x = held_ref[at, pl.ds(pl.multiple_of(half * (cols // 2) + to, wide), wide)]
                hi = x.astype(B16)
                parts_ref[half, at, pl.ds(to, wide)] = hi
                parts_ref[half, at, pl.ds(pl.multiple_of(cols // 2 + to, wide), wide)] = (x - hi.astype(F32)).astype(B16)
                x = x.T
                hi = x.astype(B16)
                down = pl.ds(pl.multiple_of(half * (cols // 2) + to, wide), wide)
                t_parts_ref[side, down, place : place + tile] = hi
                place_lo = rows // 2 + place
                t_parts_ref[side, down, place_lo : place_lo + tile] = (x - hi.astype(F32)).astype(B16)
                return 0

            lax.fori_loop(0, cols // 2 // wide, step, 0)


def half_of(ref, side):
    part = ref.shape[0] // 2
    return ref[pl.ds(pl.multiple_of(side * part, ROWS), part), :]


def two_parts(x):
    hi = x.astype(B16)
    lo = x - hi.astype(F32)
    return jnp.concatenate([hi, lo.astype(B16)], axis=1)


def add_product(parts_ref, side, rhs, base_ref, begin, out_ref, size):
    tile = min(size, TILE)
    rhs = jnp.concatenate([rhs, rhs], axis=0)

    def step(i, _):
        to = pl.multiple_of(i * tile, tile)
        at = pl.multiple_of(begin + to, tile)
        both = jnp.dot(parts_ref[side, pl.ds(at, tile), :], rhs, preferred_element_type=F32)
        rows = both[:, :LANES] + both[:, LANES:]
        if base_ref is not None:
            rows = base_ref[pl.ds(at, tile), :] + rows
        out_ref[pl.ds(to, tile), :] = rows
        return 0

    lax.fori_loop(0, size // tile, step, 0)


def block_of(rows):
    return jnp.concatenate(rows + [jnp.zeros((ROWS - len(rows), LANES), F32)], axis=0)


def column_sum(x):
    return jnp.sum(x, axis=0, keepdims=True)


def next_rows(energy, mixed, alpha, beta, r, v):
    unit = r * (1.0 / beta)
    return energy * unit + mixed - alpha * unit - beta * v, unit


def advance_own(own_ref, energy_ref, fixed_ref, y_ref, r_ref, v_ref):
    part = r_ref.shape[0]
    alpha = fixed_ref[1:2, :] + column_sum(y_ref[part:, :])
    r, unit = next_rows(
        half_of(energy_ref, own_ref[LEAD]), y_ref[:part, :], alpha, fixed_ref[0:1, :], r_ref[...], v_ref[...]
    )
    return r, unit, alpha


def advance_other(own_ref, energy_ref, fixed_ref, alpha_ref, y_ref, r_ref, v_ref):
    return next_rows(
        half_of(energy_ref, 1 - own_ref[LEAD]), y_ref[...], alpha_ref[...], fixed_ref[0:1, :], r_ref[...], v_ref[...]
    )


def first_own(own_ref, t_parts_ref, energy_ref, start_ref, base_ref, sums_ref, own_half_ref):
    r = half_of(start_ref, own_ref[LEAD])
    own_half_ref[...] = r
    project_rows(own_ref[LEAD], t_parts_ref, energy_ref, r, base_ref, sums_ref)


def project_own(own_ref, t_parts_ref, energy_ref, fixed_ref, y_ref, r_ref, v_ref, base_ref, sums_ref, next_ref, unit_ref, alpha_ref):
    r, unit_ref[...], alpha_ref[...] = advance_own(own_ref, energy_ref, fixed_ref, y_ref, r_ref, v_ref)
    next_ref[...] = r
    project_rows(own_ref[LEAD], t_parts_ref, energy_ref, r, base_ref, sums_ref)


def project_rows(side, t_parts_ref, energy_ref, r, base_ref, sums_ref):
    square = r * r
    sums_ref[...] = block_of([column_sum(square), column_sum(square * half_of(energy_ref, side))])
    add_product(t_parts_ref, side, two_parts(r), None, 0, base_ref, base_ref.shape[0])


def project_send(own_ref, t_parts_ref, energy_ref, base_ref, sums_ref, *refs, first, chips):
    side = 1 - own_ref[LEAD]
    if first:
        start_ref, send_ref, rhs_ref, tail_ref, next_ref = refs
        r = half_of(start_ref, side)
    else:
        send_ref, rhs_ref, tail_ref, next_ref, unit_ref = refs[5:]
        r, unit_ref[...] = advance_other(own_ref, energy_ref, *refs[:5])
    next_ref[...] = r
    square = r * r
    squares = sums_ref[0:1, :] + column_sum(square)
    energies = sums_ref[1:2, :] + column_sum(square * half_of(energy_ref, side))
    row = lax.broadcasted_iota(jnp.int32, tail_ref.shape, 0)
    chip = own_ref[CHIP]
    tail = jnp.where(row == chip, squares, jnp.where(row == chips + chip, energies, 0.0))
    tail_ref[...] = tail
    rhs = two_parts(r)
    rhs_ref[...] = rhs
    part = t_parts_ref.shape[1] // 2
    add_product(t_parts_ref, side, rhs, base_ref, (1 - own_ref[CORE]) * part, send_ref, part)
    send_ref[part:, :] = tail


def project_keep(own_ref, t_parts_ref, base_ref, rhs_ref, tail_ref, keep_ref):
    part = t_parts_ref.shape[1] // 2
    side = 1 - own_ref[LEAD]
    add_product(t_parts_ref, side, rhs_ref[...], base_ref, own_ref[CORE] * part, keep_ref, part)
    keep_ref[part:, :] = tail_ref[...]


def exchange_own(own_ref, parts_ref, weights_ref, held_ref, base_ref, fixed_ref, *, chips):
    part = weights_ref.shape[0] // 2
    squares = column_sum(held_ref[part : part + chips, :])
    energies = column_sum(held_ref[part + chips : part + 2 * chips, :])
    beta = jnp.sqrt(squares + EPSILON)
    inverse = 1.0 / beta
    projected = held_ref[:part, :] * inverse
    weighted = half_of(weights_ref, own_ref[CORE]) * projected
    fixed_ref[...] = block_of(
        [beta, energies * inverse * inverse, column_sum(projected * weighted)]
    )
    add_product(parts_ref, own_ref[CORE], two_parts(weighted), None, 0, base_ref, base_ref.shape[0])


def exchange_send(own_ref, parts_ref, weights_ref, base_ref, fixed_ref, other_ref, send_ref, rhs_ref, tail_ref):
    side = 1 - own_ref[CORE]
    projected = other_ref[...] * (1.0 / fixed_ref[0:1, :])
    weighted = half_of(weights_ref, side) * projected
    other = column_sum(projected * weighted)
    mine = fixed_ref[2:3, :]
    curvature = jnp.where(own_ref[CORE] == 0, mine + other, other + mine)
    row = lax.broadcasted_iota(jnp.int32, tail_ref.shape, 0)
    tail = jnp.where(row == own_ref[DEPTH], curvature, 0.0)
    tail_ref[...] = tail
    rhs = two_parts(weighted)
    rhs_ref[...] = rhs
    part = parts_ref.shape[1] // 2
    add_product(parts_ref, side, rhs, base_ref, (1 - own_ref[LEAD]) * part, send_ref, part)
    send_ref[part:, :] = tail


def exchange_keep(own_ref, parts_ref, base_ref, rhs_ref, tail_ref, keep_ref):
    part = parts_ref.shape[1] // 2
    side = 1 - own_ref[CORE]
    add_product(parts_ref, side, rhs_ref[...], base_ref, own_ref[LEAD] * part, keep_ref, part)
    keep_ref[part:, :] = tail_ref[...]


def finish_own(own_ref, energy_ref, fixed_ref, y_ref, r_ref, v_ref, next_ref, square_ref, alpha_ref):
    r, _, alpha_ref[...] = advance_own(own_ref, energy_ref, fixed_ref, y_ref, r_ref, v_ref)
    next_ref[...] = r
    square_ref[...] = block_of([column_sum(r * r)])


def finish_other(own_ref, energy_ref, fixed_ref, alpha_ref, y_ref, r_ref, v_ref, own_half_ref, out_ref):
    side = own_ref[LEAD]
    part = own_half_ref.shape[0]
    other, _ = advance_other(own_ref, energy_ref, fixed_ref, alpha_ref, y_ref, r_ref, v_ref)
    out_ref[pl.ds(pl.multiple_of(side * part, ROWS), part), :] = own_half_ref[...]
    out_ref[pl.ds(pl.multiple_of((1 - side) * part, ROWS), part), :] = other


def swaps(size, bit):
    return [(i, i ^ bit) for i in range(size)]


def bits_of(size):
    return [1 << b for b in range(size.bit_length() - 1)]


def crossed_swaps(size):
    bits = bits_of(size)[1:]
    turned = bits[::-1]
    return [
        [(i, i ^ (turned[n] if i & 1 else bits[n])) for i in range(size)] for n in range(len(bits))
    ]


def depth_swaps(ka, ga):
    bits = bits_of(ga)
    orders = [bits, bits[1:2] + bits[:1] + bits[2:]]
    return [
        [(a * ga + g, a * ga + (g ^ orders[a & 1][n])) for a in range(ka) for g in range(ga)]
        for n in range(len(bits))
    ]


def chunks(size, cuts):
    edges = [0] + [size * c // 16 // ROWS * ROWS for c in cuts] + [None]
    return [slice(*pair) for pair in zip(edges[:-1], edges[1:])][::-1]


def size_of(at, size):
    return (size if at.stop is None else at.stop) - at.start


def joined(pieces):
    return [jnp.concatenate(part, axis=0) for part in zip(*pieces)]


def per_device(ka, ga, pair_densities, energies, coulomb, start):
    rows, cols = pair_densities.shape
    half_r, half_g = rows // 2, cols // 2
    chips = ka // 2
    s_rows = -(-2 * chips // ROWS) * ROWS
    z_rows = -(-ga // ROWS) * ROWS
    core, chip, depth = lax.axis_index("ka") & 1, lax.axis_index("ka") >> 1, lax.axis_index("ga")
    lead = jnp.where(core == 0, depth & 1, (depth >> 1) & 1)
    own = jnp.stack([core, lead, depth, chip]).astype(jnp.int32)
    parts, t_parts = pl.pallas_call(
        split_matrix,
        out_shape=[
            jax.ShapeDtypeStruct((2, rows, cols), B16),
            jax.ShapeDtypeStruct((2, cols, rows), B16),
        ],
        in_specs=[SMEM, pl.BlockSpec(memory_space=pltpu.HBM)],
        out_specs=[VMEM] * 2,
        scratch_shapes=[
            pltpu.VMEM((rows, cols), F32),
            pltpu.SemaphoreType.DMA((rows // min(half_r, 128),)),
        ],
        cost_estimate=pl.CostEstimate(flops=2**31, bytes_accessed=0, transcendentals=0),
        compiler_params=pltpu.CompilerParams(vmem_limit_bytes=34 * MIB),
    )(own, pair_densities)
    energy = jnp.broadcast_to(energies[:, None], (rows, LANES))
    weights = jnp.broadcast_to(coulomb[:, None], (cols, LANES))

    flops = rows * cols * LANES * 4
    line, block, half = ((1, LANES), F32), ((ROWS, LANES), F32), ((half_r, LANES), F32)
    wide = 2 * LANES
    both = ("ka", "ga")
    first_round, *rounds = depth_swaps(ka, ga)

    alphas, betas = [], []
    r = v = fixed = y_own = y_other = None
    for step in range(ITERS):
        outs = [((half_g + s_rows, LANES), F32), ((half_r, wide), B16), ((s_rows, LANES), F32)]
        if step == 0:
            base, sums, r_own = call(
                first_own, [((cols, LANES), F32), block, half], flops // 2, own, t_parts, energy, start
            )
            send, rhs, tail, r_other = call(
                functools.partial(project_send, first=True, chips=chips),
                outs + [half],
                flops // 4,
                own,
                t_parts,
                energy,
                base,
                sums,
                start,
            )
            r = (r_own, r_other)
            v = (jnp.zeros_like(r_own),) * 2
        else:
            base, sums, r_own, v_own, alpha = call(
                project_own,
                [((cols, LANES), F32), block, half, half, line],
                flops // 2,
                own,
                t_parts,
                energy,
                fixed,
                y_own,
                r[0],
                v[0],
            )
            send, rhs, tail, r_other, v_other = call(
                functools.partial(project_send, first=False, chips=chips),
                outs + [half, half],
                flops // 4,
                own,
                t_parts,
                energy,
                base,
                sums,
                fixed,
                alpha,
                y_other,
                r[1],
                v[1],
            )
            r, v = (r_own, r_other), (v_own, v_other)
            alphas.append(alpha)
        arrived = lax.ppermute(send, "ka", swaps(ka, 1))
        (keep,) = call(project_keep, outs[:1], flops // 4, own, t_parts, base, rhs, tail)
        pieces = []
        for at in chunks(half_g, KA_CUTS):
            held = keep[at] + arrived[at]
            for pairs in crossed_swaps(ka):
                held = held + lax.ppermute(held, "ka", pairs)
            pieces.insert(0, (held, lax.ppermute(held[: size_of(at, half_g)], "ka", swaps(ka, 1))))
        held, other = joined(pieces)
        base, fixed = call(
            functools.partial(exchange_own, chips=chips),
            [((rows, LANES), F32), block],
            flops // 2,
            own,
            parts,
            weights,
            held,
        )
        if step > 0:
            betas.append(fixed[0:1])
        outs = [((half_r + z_rows, LANES), F32), ((half_g, wide), B16), ((z_rows, LANES), F32)]
        send, rhs, tail = call(exchange_send, outs, flops // 4, own, parts, weights, base, fixed, other)
        pieces = []
        arrived = [
            lax.ppermute(send[at], both, first_round) for at in chunks(half_r, GA_CUTS)
        ]
        (keep,) = call(exchange_keep, outs[:1], flops // 4, own, parts, base, rhs, tail)
        for at, part in zip(chunks(half_r, GA_CUTS), arrived):
            y_own = keep[at] + part
            for pairs in rounds:
                y_own = y_own + lax.ppermute(y_own, both, pairs)
            pieces.insert(0, (y_own, lax.ppermute(y_own[: size_of(at, half_r)], both, first_round)))
        y_own, y_other = joined(pieces)
    r_own, square, alpha = call(finish_own, [half, block, line], 2**20, own, energy, fixed, y_own, r[0], v[0])
    alphas.append(alpha)
    square = square + lax.ppermute(square, both, first_round)
    for bit in bits_of(ka):
        square = square + lax.ppermute(square, "ka", swaps(ka, bit))
    (last,) = call(
        finish_other,
        [((rows, LANES), F32)],
        2**20,
        own,
        energy,
        fixed,
        alpha,
        y_other,
        r[1],
        v[1],
        r_own,
    )
    beta = jnp.sqrt(square[0:1] + EPSILON)
    betas.append(beta)
    return (
        jnp.concatenate(alphas, axis=0),
        jnp.concatenate(betas, axis=0),
        last / beta,
    )


def solution(mesh):
    placed = (P("ka", "ga"), P("ka"), P("ga"), P("ka", None))
    return jax.shard_map(
        functools.partial(per_device, mesh.shape["ka"], mesh.shape["ga"]),
        mesh=mesh,
        in_specs=placed,
        out_specs=(P(), P(), P("ka", None)),
        check_vma=False,
    )
```

```python
import functools

import jax
import jax.numpy as jnp
from jax import lax
from jax.experimental import pallas as pl
from jax.experimental.pallas import tpu as pltpu
from jax.sharding import PartitionSpec as P


ITERS = 4
EPSILON = 1e-06
LANES = 128
KA_CUT = 6
GA_CUTS = (8,)
ROWS = 8
MIB = 1024 * 1024


VMEM = pl.BlockSpec(memory_space=pltpu.VMEM)
SMEM = pl.BlockSpec(memory_space=pltpu.SMEM)
F32, B16 = jnp.float32, jnp.bfloat16

CORE, LEAD, DEPTH, CHIP = range(4)


def call(body, outs, flops, own, *args):
    return pl.pallas_call(
        body,
        out_shape=[jax.ShapeDtypeStruct(shape, dtype) for shape, dtype in outs],
        in_specs=[SMEM] + [VMEM] * len(args),
        out_specs=[VMEM] * len(outs),
        cost_estimate=pl.CostEstimate(flops=flops, bytes_accessed=0, transcendentals=0),
        compiler_params=pltpu.CompilerParams(vmem_limit_bytes=8 * MIB),
    )(own, *args)


def split_matrix(own_ref, m_ref, parts_ref, t_parts_ref, held_ref, arrived):
    rows, cols = m_ref.shape
    tile = min(rows // 2, 128)
    wide = min(cols // 2, 1024)
    copies = []
    for i in range(rows // tile):
        at = pl.ds(i * tile, tile)
        copies.append(pltpu.make_async_copy(m_ref.at[at, :], held_ref.at[at, :], arrived.at[i]))
        copies[-1].start()
    for i in range(rows // tile):
        at = pl.ds(i * tile, tile)
        side, place = divmod(i * tile, rows // 2)
        copies[i].wait()
        for half in range(2):

            def step(j, _):
                to = pl.multiple_of(j * wide, wide)
                x = held_ref[at, pl.ds(pl.multiple_of(half * (cols // 2) + to, wide), wide)]
                hi = x.astype(B16)
                parts_ref[half, at, pl.ds(to, wide)] = hi
                parts_ref[half, at, pl.ds(pl.multiple_of(cols // 2 + to, wide), wide)] = (x - hi.astype(F32)).astype(B16)
                x = x.T
                hi = x.astype(B16)
                down = pl.ds(pl.multiple_of(half * (cols // 2) + to, wide), wide)
                t_parts_ref[side, down, place : place + tile] = hi
                place_lo = rows // 2 + place
                t_parts_ref[side, down, place_lo : place_lo + tile] = (x - hi.astype(F32)).astype(B16)
                return 0

            lax.fori_loop(0, cols // 2 // wide, step, 0)


def half_of(ref, side):
    part = ref.shape[0] // 2
    return ref[pl.ds(pl.multiple_of(side * part, ROWS), part), :]


def two_parts(x):
    hi = x.astype(B16)
    lo = x - hi.astype(F32)
    return jnp.concatenate([hi, lo.astype(B16)], axis=1)


def columns_product(parts_ref, side, rhs):
    both = jnp.dot(parts_ref[side], jnp.concatenate([rhs, rhs], axis=0), preferred_element_type=F32)
    return both[:, :LANES] + both[:, LANES:]


def add_product(parts_ref, side, rhs, base_ref, begin, out_ref, size):
    rows = pl.ds(pl.multiple_of(begin, ROWS), size)
    rhs = jnp.concatenate([rhs, rhs], axis=0)
    both = jnp.dot(parts_ref[side, rows, :], rhs, preferred_element_type=F32)
    out_ref[:size, :] = base_ref[rows, :] + (both[:, :LANES] + both[:, LANES:])


def block_of(rows):
    return jnp.concatenate(rows + [jnp.zeros((ROWS - len(rows), LANES), F32)], axis=0)


def column_sum(x):
    return jnp.sum(x, axis=0, keepdims=True)


def next_rows(energy, mixed, alpha, beta, r, v):
    unit = r * (1.0 / beta)
    return energy * unit + mixed - alpha * unit - beta * v, unit


def advance_own(own_ref, energy_ref, fixed_ref, y_ref, r_ref, v_ref):
    part = r_ref.shape[0]
    alpha = fixed_ref[1:2, :] + column_sum(y_ref[part:, :])
    r, unit = next_rows(
        half_of(energy_ref, own_ref[LEAD]), y_ref[:part, :], alpha, fixed_ref[0:1, :], r_ref[...], v_ref[...]
    )
    return r, unit, alpha


def advance_other(own_ref, energy_ref, fixed_ref, alpha_ref, y_ref, r_ref, v_ref):
    return next_rows(
        half_of(energy_ref, 1 - own_ref[LEAD]), y_ref[...], alpha_ref[...], fixed_ref[0:1, :], r_ref[...], v_ref[...]
    )


def add_both(t_parts_ref, lead, rhs_ref, begin, out_ref, size):
    rows = pl.ds(begin, size)
    total = None
    for n, side in enumerate((lead, 1 - lead)):
        rhs = jnp.concatenate([rhs_ref[n]] * 2, axis=0)
        both = jnp.dot(t_parts_ref[side, rows, :], rhs, preferred_element_type=F32)
        total = both if total is None else total + both
    out_ref[:size, :] = total[:, :LANES] + total[:, LANES:]


def first_send(own_ref, t_parts_ref, energy_ref, start_ref, send_ref, rhs_ref, tail_ref, own_half_ref, other_half_ref, *, chips):
    lead = own_ref[LEAD]
    squares = energies = 0.0
    for n, (side, ref) in enumerate(((lead, own_half_ref), (1 - lead, other_half_ref))):
        r = half_of(start_ref, side)
        ref[...] = r
        rhs_ref[n] = two_parts(r)
        squares = squares + column_sum(r * r)
        energies = energies + column_sum(r * r * half_of(energy_ref, side))
    tail = tail_of(own_ref, tail_ref.shape, squares, energies, chips)
    tail_ref[...] = tail
    part = t_parts_ref.shape[1] // 2
    begin = pl.multiple_of((1 - own_ref[CORE]) * part, ROWS)
    add_both(t_parts_ref, lead, rhs_ref, begin, send_ref, part)
    send_ref[part:, :] = tail


def first_keep(own_ref, t_parts_ref, rhs_ref, tail_ref, keep_ref):
    part = t_parts_ref.shape[1] // 2
    begin = pl.multiple_of(own_ref[CORE] * part, ROWS)
    add_both(t_parts_ref, own_ref[LEAD], rhs_ref, begin, keep_ref, part)
    keep_ref[part:, :] = tail_ref[...]


def tail_of(own_ref, shape, squares, energies, chips):
    row = lax.broadcasted_iota(jnp.int32, shape, 0)
    chip = own_ref[CHIP]
    return jnp.where(row == chip, squares, jnp.where(row == chips + chip, energies, 0.0))


def project_own(own_ref, t_parts_ref, energy_ref, fixed_ref, y_ref, r_ref, v_ref, base_ref, sums_ref, next_ref, unit_ref, alpha_ref):
    r, unit_ref[...], alpha_ref[...] = advance_own(own_ref, energy_ref, fixed_ref, y_ref, r_ref, v_ref)
    next_ref[...] = r
    project_rows(own_ref[LEAD], t_parts_ref, energy_ref, r, base_ref, sums_ref)


def project_rows(side, t_parts_ref, energy_ref, r, base_ref, sums_ref):
    square = r * r
    sums_ref[...] = block_of([column_sum(square), column_sum(square * half_of(energy_ref, side))])
    base_ref[...] = columns_product(t_parts_ref, side, two_parts(r))


def project_send(own_ref, t_parts_ref, energy_ref, base_ref, sums_ref, fixed_ref, alpha_ref, y_ref, r_ref, v_ref, send_ref, rhs_ref, tail_ref, next_ref, unit_ref, *, chips):
    side = 1 - own_ref[LEAD]
    r, unit_ref[...] = advance_other(own_ref, energy_ref, fixed_ref, alpha_ref, y_ref, r_ref, v_ref)
    next_ref[...] = r
    square = r * r
    squares = sums_ref[0:1, :] + column_sum(square)
    energies = sums_ref[1:2, :] + column_sum(square * half_of(energy_ref, side))
    tail = tail_of(own_ref, tail_ref.shape, squares, energies, chips)
    tail_ref[...] = tail
    rhs = two_parts(r)
    rhs_ref[...] = rhs
    part = t_parts_ref.shape[1] // 2
    add_product(t_parts_ref, side, rhs, base_ref, (1 - own_ref[CORE]) * part, send_ref, part)
    send_ref[part:, :] = tail


def project_keep(own_ref, t_parts_ref, base_ref, rhs_ref, tail_ref, keep_ref):
    part = t_parts_ref.shape[1] // 2
    side = 1 - own_ref[LEAD]
    add_product(t_parts_ref, side, rhs_ref[...], base_ref, own_ref[CORE] * part, keep_ref, part)
    keep_ref[part:, :] = tail_ref[...]


def exchange_own(own_ref, parts_ref, weights_ref, held_ref, base_ref, fixed_ref, *, chips):
    part = weights_ref.shape[0] // 2
    squares = column_sum(held_ref[part : part + chips, :])
    energies = column_sum(held_ref[part + chips : part + 2 * chips, :])
    beta = jnp.sqrt(squares + EPSILON)
    inverse = 1.0 / beta
    projected = held_ref[:part, :] * inverse
    weighted = half_of(weights_ref, own_ref[CORE]) * projected
    fixed_ref[...] = block_of(
        [beta, energies * inverse * inverse, column_sum(projected * weighted)]
    )
    base_ref[...] = columns_product(parts_ref, own_ref[CORE], two_parts(weighted))


def exchange_send(own_ref, parts_ref, weights_ref, base_ref, fixed_ref, other_ref, send_ref, rhs_ref, tail_ref):
    side = 1 - own_ref[CORE]
    projected = other_ref[...] * (1.0 / fixed_ref[0:1, :])
    weighted = half_of(weights_ref, side) * projected
    other = column_sum(projected * weighted)
    mine = fixed_ref[2:3, :]
    curvature = jnp.where(own_ref[CORE] == 0, mine + other, other + mine)
    row = lax.broadcasted_iota(jnp.int32, tail_ref.shape, 0)
    tail = jnp.where(row == own_ref[DEPTH], curvature, 0.0)
    tail_ref[...] = tail
    rhs = two_parts(weighted)
    rhs_ref[...] = rhs
    part = parts_ref.shape[1] // 2
    add_product(parts_ref, side, rhs, base_ref, (1 - own_ref[LEAD]) * part, send_ref, part)
    send_ref[part:, :] = tail


def exchange_keep(own_ref, parts_ref, base_ref, rhs_ref, tail_ref, keep_ref):
    part = parts_ref.shape[1] // 2
    side = 1 - own_ref[CORE]
    add_product(parts_ref, side, rhs_ref[...], base_ref, own_ref[LEAD] * part, keep_ref, part)
    keep_ref[part:, :] = tail_ref[...]


def finish_own(own_ref, energy_ref, fixed_ref, y_ref, r_ref, v_ref, next_ref, square_ref, alpha_ref):
    r, _, alpha_ref[...] = advance_own(own_ref, energy_ref, fixed_ref, y_ref, r_ref, v_ref)
    next_ref[...] = r
    square_ref[...] = block_of([column_sum(r * r)])


def finish_other(own_ref, energy_ref, fixed_ref, alpha_ref, y_ref, r_ref, v_ref, own_half_ref, out_ref):
    side = own_ref[LEAD]
    part = own_half_ref.shape[0]
    other, _ = advance_other(own_ref, energy_ref, fixed_ref, alpha_ref, y_ref, r_ref, v_ref)
    out_ref[pl.ds(pl.multiple_of(side * part, ROWS), part), :] = own_half_ref[...]
    out_ref[pl.ds(pl.multiple_of((1 - side) * part, ROWS), part), :] = other


def swaps(size, bit):
    return [(i, i ^ bit) for i in range(size)]


def bits_of(size):
    return [1 << b for b in range(size.bit_length() - 1)]


def crossed_swaps(size):
    bits = bits_of(size)[1:]
    turned = bits[::-1]
    return [
        [(i, i ^ (turned[n] if i & 1 else bits[n])) for i in range(size)] for n in range(len(bits))
    ]


def depth_swaps(ka, ga):
    bits = bits_of(ga)
    orders = [bits, bits[1:2] + bits[:1] + bits[2:]]
    return [
        [(a * ga + g, a * ga + (g ^ orders[a & 1][n])) for a in range(ka) for g in range(ga)]
        for n in range(len(bits))
    ]


def chunks(size, cuts):
    edges = [0] + [size * c // 16 // ROWS * ROWS for c in cuts] + [None]
    return [slice(*pair) for pair in zip(edges[:-1], edges[1:])][::-1]


def size_of(at, size):
    return (size if at.stop is None else at.stop) - at.start


def joined(pieces):
    return [jnp.concatenate(part, axis=0) for part in zip(*pieces)]


def per_device(ka, ga, pair_densities, energies, coulomb, start):
    rows, cols = pair_densities.shape
    half_r, half_g = rows // 2, cols // 2
    chips = ka // 2
    s_rows = -(-2 * chips // ROWS) * ROWS
    z_rows = -(-ga // ROWS) * ROWS
    core, chip, depth = lax.axis_index("ka") & 1, lax.axis_index("ka") >> 1, lax.axis_index("ga")
    lead = jnp.where(core == 0, depth & 1, (depth >> 1) & 1)
    own = jnp.stack([core, lead, depth, chip]).astype(jnp.int32)
    parts, t_parts = pl.pallas_call(
        split_matrix,
        out_shape=[
            jax.ShapeDtypeStruct((2, rows, cols), B16),
            jax.ShapeDtypeStruct((2, cols, rows), B16),
        ],
        in_specs=[SMEM, pl.BlockSpec(memory_space=pltpu.HBM)],
        out_specs=[VMEM] * 2,
        scratch_shapes=[
            pltpu.VMEM((rows, cols), F32),
            pltpu.SemaphoreType.DMA((rows // min(half_r, 128),)),
        ],
        cost_estimate=pl.CostEstimate(flops=2**31, bytes_accessed=0, transcendentals=0),
        compiler_params=pltpu.CompilerParams(vmem_limit_bytes=34 * MIB),
    )(own, pair_densities)
    energy = jnp.broadcast_to(energies[:, None], (rows, LANES))
    weights = jnp.broadcast_to(coulomb[:, None], (cols, LANES))

    flops = rows * cols * LANES * 4
    edge = half_g * KA_CUT // 16 // LANES * LANES or LANES
    line, block, half = ((1, LANES), F32), ((ROWS, LANES), F32), ((half_r, LANES), F32)
    wide = 2 * LANES
    both = ("ka", "ga")
    first_round, *rounds = depth_swaps(ka, ga)

    alphas, betas = [], []
    r = v = fixed = y_own = y_other = None
    for step in range(ITERS):
        outs = [((half_g + s_rows, LANES), F32), ((half_r, wide), B16), ((s_rows, LANES), F32)]
        if step == 0:
            outs[1] = ((2, half_r, wide), B16)
            send, rhs, tail, *r = call(
                functools.partial(first_send, chips=chips),
                outs + [half, half],
                flops // 2,
                own,
                t_parts,
                energy,
                start,
            )
            v = (jnp.zeros_like(r[0]),) * 2
        else:
            base, sums, r_own, v_own, alpha = call(
                project_own,
                [((cols, LANES), F32), block, half, half, line],
                flops // 2,
                own,
                t_parts,
                energy,
                fixed,
                y_own,
                r[0],
                v[0],
            )
            send, rhs, tail, r_other, v_other = call(
                functools.partial(project_send, chips=chips),
                outs + [half, half],
                flops // 4,
                own,
                t_parts,
                energy,
                base,
                sums,
                fixed,
                alpha,
                y_other,
                r[1],
                v[1],
            )
            r, v = (r_own, r_other), (v_own, v_other)
            alphas.append(alpha)
        arrived = lax.ppermute(send, "ka", swaps(ka, 1))
        if step == 0:
            (keep,) = call(first_keep, outs[:1], flops // 2, own, t_parts, rhs, tail)
        else:
            (keep,) = call(project_keep, outs[:1], flops // 4, own, t_parts, base, rhs, tail)
        pieces = []
        for at in (slice(edge, None), slice(0, edge)):
            held = keep[at] + arrived[at]
            for pairs in crossed_swaps(ka):
                held = held + lax.ppermute(held, "ka", pairs)
            pieces.insert(0, (held, lax.ppermute(held[: size_of(at, half_g)], "ka", swaps(ka, 1))))
        held, other = joined(pieces)
        base, fixed = call(
            functools.partial(exchange_own, chips=chips),
            [((rows, LANES), F32), block],
            flops // 2,
            own,
            parts,
            weights,
            held,
        )
        if step > 0:
            betas.append(fixed[0:1])
        outs = [((half_r + z_rows, LANES), F32), ((half_g, wide), B16), ((z_rows, LANES), F32)]
        send, rhs, tail = call(exchange_send, outs, flops // 4, own, parts, weights, base, fixed, other)
        pieces = []
        arrived = [
            lax.ppermute(send[at], both, first_round) for at in chunks(half_r, GA_CUTS)
        ]
        (keep,) = call(exchange_keep, outs[:1], flops // 4, own, parts, base, rhs, tail)
        for at, part in zip(chunks(half_r, GA_CUTS), arrived):
            y_own = keep[at] + part
            for pairs in rounds:
                y_own = y_own + lax.ppermute(y_own, both, pairs)
            y_part = y_own[: size_of(at, half_r)]
            y_part = lax.ppermute(y_part, both, first_round)
            pieces.insert(0, (y_own, y_part))
        y_own, y_other = joined(pieces)
    r_own, square, alpha = call(finish_own, [half, block, line], 2**20, own, energy, fixed, y_own, r[0], v[0])
    alphas.append(alpha)
    came = lax.ppermute(square, both, first_round)
    square = square + came
    for bit in bits_of(ka):
        came = lax.ppermute(square, "ka", swaps(ka, bit))
        square = square + came
    (last,) = call(
        finish_other,
        [((rows, LANES), F32)],
        flops // 4,
        own,
        energy,
        fixed,
        alpha,
        y_other,
        r[1],
        v[1],
        r_own,
    )
    beta = jnp.sqrt(square[0:1] + EPSILON)
    betas.append(beta)
    return (
        jnp.concatenate(alphas, axis=0),
        jnp.concatenate(betas, axis=0),
        last / beta,
    )


def solution(mesh):
    placed = (P("ka", "ga"), P("ka"), P("ga"), P("ka", None))
    return jax.shard_map(
        functools.partial(per_device, mesh.shape["ka"], mesh.shape["ga"]),
        mesh=mesh,
        in_specs=placed,
        out_specs=(P(), P(), P("ka", None)),
        check_vma=False,
    )
```

```python
import functools

import jax
import jax.numpy as jnp
from jax import lax
from jax.experimental import pallas as pl
from jax.experimental.pallas import tpu as pltpu
from jax.sharding import PartitionSpec as P


ITERS = 4
EPSILON = 1e-06
LANES = 128
KA_CUT = 6
GA_CUTS = (8,)
ROWS = 8
MIB = 1024 * 1024


VMEM = pl.BlockSpec(memory_space=pltpu.VMEM)
SMEM = pl.BlockSpec(memory_space=pltpu.SMEM)
F32, B16 = jnp.float32, jnp.bfloat16

CORE, LEAD, DEPTH, CHIP = range(4)


def call(body, outs, flops, own, *args):
    return pl.pallas_call(
        body,
        out_shape=[jax.ShapeDtypeStruct(shape, dtype) for shape, dtype in outs],
        in_specs=[SMEM] + [VMEM] * len(args),
        out_specs=[VMEM] * len(outs),
        cost_estimate=pl.CostEstimate(flops=flops, bytes_accessed=0, transcendentals=0),
        compiler_params=pltpu.CompilerParams(vmem_limit_bytes=8 * MIB),
    )(own, *args)


def split_matrix(own_ref, m_ref, parts_ref, t_parts_ref, held_ref, arrived):
    rows, cols = m_ref.shape
    tile = min(rows // 2, 128)
    wide = min(cols // 2, 1024)
    copies = []
    for i in range(rows // tile):
        at = pl.ds(i * tile, tile)
        copies.append(pltpu.make_async_copy(m_ref.at[at, :], held_ref.at[at, :], arrived.at[i]))
        copies[-1].start()
    for i in range(rows // tile):
        at = pl.ds(i * tile, tile)
        side, place = divmod(i * tile, rows // 2)
        copies[i].wait()
        for half in range(2):

            def step(j, _):
                to = pl.multiple_of(j * wide, wide)
                x = held_ref[at, pl.ds(pl.multiple_of(half * (cols // 2) + to, wide), wide)]
                hi = x.astype(B16)
                parts_ref[half, at, pl.ds(to, wide)] = hi
                parts_ref[half, at, pl.ds(pl.multiple_of(cols // 2 + to, wide), wide)] = (x - hi.astype(F32)).astype(B16)
                x = x.T
                hi = x.astype(B16)
                down = pl.ds(pl.multiple_of(half * (cols // 2) + to, wide), wide)
                t_parts_ref[side, down, place : place + tile] = hi
                place_lo = rows // 2 + place
                t_parts_ref[side, down, place_lo : place_lo + tile] = (x - hi.astype(F32)).astype(B16)
                return 0

            lax.fori_loop(0, cols // 2 // wide, step, 0)


def half_of(ref, side):
    part = ref.shape[0] // 2
    return ref[pl.ds(pl.multiple_of(side * part, ROWS), part), :]


def two_parts(x):
    hi = x.astype(B16)
    lo = x - hi.astype(F32)
    return jnp.concatenate([hi, lo.astype(B16)], axis=1)


def columns_product(parts_ref, side, begin, rhs):
    width = rhs.shape[0]
    low = parts_ref.shape[2] // 2 + begin
    if 2 * width == parts_ref.shape[2]:
        matrix = parts_ref[side]
    else:
        matrix = jnp.concatenate(
            [parts_ref[side, :, begin : begin + width], parts_ref[side, :, low : low + width]], axis=1
        )
    both = jnp.dot(matrix, jnp.concatenate([rhs, rhs], axis=0), preferred_element_type=F32)
    return both[:, :LANES] + both[:, LANES:]


def add_product(parts_ref, side, rhs, base_ref, begin, out_ref, size):
    rows = pl.ds(pl.multiple_of(begin, ROWS), size)
    rhs = jnp.concatenate([rhs, rhs], axis=0)
    both = jnp.dot(parts_ref[side, rows, :], rhs, preferred_element_type=F32)
    out_ref[:size, :] = base_ref[rows, :] + (both[:, :LANES] + both[:, LANES:])


def block_of(rows):
    return jnp.concatenate(rows + [jnp.zeros((ROWS - len(rows), LANES), F32)], axis=0)


def column_sum(x):
    return jnp.sum(x, axis=0, keepdims=True)


def next_rows(energy, mixed, alpha, beta, r, v):
    unit = r * (1.0 / beta)
    return energy * unit + mixed - alpha * unit - beta * v, unit


def advance_own(own_ref, energy_ref, fixed_ref, y_ref, r_ref, v_ref):
    part = r_ref.shape[0]
    alpha = fixed_ref[1:2, :] + column_sum(y_ref[part:, :])
    r, unit = next_rows(
        half_of(energy_ref, own_ref[LEAD]), y_ref[:part, :], alpha, fixed_ref[0:1, :], r_ref[...], v_ref[...]
    )
    return r, unit, alpha


def advance_other(own_ref, energy_ref, fixed_ref, alpha_ref, y_ref, r_ref, v_ref):
    return next_rows(
        half_of(energy_ref, 1 - own_ref[LEAD]), y_ref[...], alpha_ref[...], fixed_ref[0:1, :], r_ref[...], v_ref[...]
    )


def add_both(t_parts_ref, lead, rhs_ref, begin, out_ref, size):
    rows = pl.ds(begin, size)
    total = None
    for n, side in enumerate((lead, 1 - lead)):
        rhs = jnp.concatenate([rhs_ref[n]] * 2, axis=0)
        both = jnp.dot(t_parts_ref[side, rows, :], rhs, preferred_element_type=F32)
        total = both if total is None else total + both
    out_ref[:size, :] = total[:, :LANES] + total[:, LANES:]


def first_send(own_ref, t_parts_ref, energy_ref, start_ref, send_ref, rhs_ref, tail_ref, own_half_ref, other_half_ref, *, chips):
    lead = own_ref[LEAD]
    squares = energies = 0.0
    for n, (side, ref) in enumerate(((lead, own_half_ref), (1 - lead, other_half_ref))):
        r = half_of(start_ref, side)
        ref[...] = r
        rhs_ref[n] = two_parts(r)
        squares = squares + column_sum(r * r)
        energies = energies + column_sum(r * r * half_of(energy_ref, side))
    tail = tail_of(own_ref, tail_ref.shape, squares, energies, chips)
    tail_ref[...] = tail
    part = t_parts_ref.shape[1] // 2
    begin = pl.multiple_of((1 - own_ref[CORE]) * part, ROWS)
    add_both(t_parts_ref, lead, rhs_ref, begin, send_ref, part)
    send_ref[part:, :] = tail


def first_keep(own_ref, t_parts_ref, rhs_ref, tail_ref, keep_ref):
    part = t_parts_ref.shape[1] // 2
    begin = pl.multiple_of(own_ref[CORE] * part, ROWS)
    add_both(t_parts_ref, own_ref[LEAD], rhs_ref, begin, keep_ref, part)
    keep_ref[part:, :] = tail_ref[...]


def tail_of(own_ref, shape, squares, energies, chips):
    row = lax.broadcasted_iota(jnp.int32, shape, 0)
    chip = own_ref[CHIP]
    return jnp.where(row == chip, squares, jnp.where(row == chips + chip, energies, 0.0))


def project_own(own_ref, t_parts_ref, energy_ref, fixed_ref, y_ref, r_ref, v_ref, base_ref, sums_ref, next_ref, unit_ref, alpha_ref):
    r, unit_ref[...], alpha_ref[...] = advance_own(own_ref, energy_ref, fixed_ref, y_ref, r_ref, v_ref)
    next_ref[...] = r
    project_rows(own_ref[LEAD], t_parts_ref, energy_ref, r, base_ref, sums_ref)


def project_rows(side, t_parts_ref, energy_ref, r, base_ref, sums_ref):
    square = r * r
    sums_ref[...] = block_of([column_sum(square), column_sum(square * half_of(energy_ref, side))])
    base_ref[...] = columns_product(t_parts_ref, side, 0, two_parts(r))


def project_send(own_ref, t_parts_ref, energy_ref, base_ref, sums_ref, fixed_ref, alpha_ref, y_ref, r_ref, v_ref, send_ref, rhs_ref, tail_ref, next_ref, unit_ref, *, chips):
    side = 1 - own_ref[LEAD]
    r, unit_ref[...] = advance_other(own_ref, energy_ref, fixed_ref, alpha_ref, y_ref, r_ref, v_ref)
    next_ref[...] = r
    square = r * r
    squares = sums_ref[0:1, :] + column_sum(square)
    energies = sums_ref[1:2, :] + column_sum(square * half_of(energy_ref, side))
    tail = tail_of(own_ref, tail_ref.shape, squares, energies, chips)
    tail_ref[...] = tail
    rhs = two_parts(r)
    rhs_ref[...] = rhs
    part = t_parts_ref.shape[1] // 2
    add_product(t_parts_ref, side, rhs, base_ref, (1 - own_ref[CORE]) * part, send_ref, part)
    send_ref[part:, :] = tail


def project_keep(own_ref, t_parts_ref, base_ref, rhs_ref, tail_ref, keep_ref):
    part = t_parts_ref.shape[1] // 2
    side = 1 - own_ref[LEAD]
    add_product(t_parts_ref, side, rhs_ref[...], base_ref, own_ref[CORE] * part, keep_ref, part)
    keep_ref[part:, :] = tail_ref[...]


def weighted_rows(weights_ref, side, begin, projected):
    at = side * (weights_ref.shape[0] // 2) + begin
    return weights_ref[pl.ds(pl.multiple_of(at, ROWS), projected.shape[0]), :] * projected


def exchange_first(own_ref, parts_ref, weights_ref, held_ref, base_ref, fixed_ref, *, chips, edge):
    part = weights_ref.shape[0] // 2 - edge
    squares = column_sum(held_ref[part : part + chips, :])
    energies = column_sum(held_ref[part + chips : part + 2 * chips, :])
    beta = jnp.sqrt(squares + EPSILON)
    inverse = 1.0 / beta
    projected = held_ref[:part, :] * inverse
    weighted = weighted_rows(weights_ref, own_ref[CORE], edge, projected)
    fixed_ref[...] = block_of(
        [beta, energies * inverse * inverse, column_sum(projected * weighted)]
    )
    base_ref[...] = columns_product(parts_ref, own_ref[CORE], edge, two_parts(weighted))


def exchange_more(own_ref, parts_ref, weights_ref, held_ref, first_ref, sums_ref, base_ref, fixed_ref):
    projected = held_ref[...] * (1.0 / sums_ref[0:1, :])
    weighted = weighted_rows(weights_ref, own_ref[CORE], 0, projected)
    total = sums_ref[2:3, :] + column_sum(projected * weighted)
    fixed_ref[...] = block_of([sums_ref[0:1, :], sums_ref[1:2, :], total])
    base_ref[...] = first_ref[...] + columns_product(parts_ref, own_ref[CORE], 0, two_parts(weighted))


def exchange_send(own_ref, parts_ref, weights_ref, base_ref, fixed_ref, other_ref, send_ref, rhs_ref, tail_ref, *, edge):
    side = 1 - own_ref[CORE]
    projected = other_ref[...] * (1.0 / fixed_ref[0:1, :])
    weighted = weighted_rows(weights_ref, side, 0, projected)
    terms = projected * weighted
    other = column_sum(terms[edge:, :]) + column_sum(terms[:edge, :])
    mine = fixed_ref[2:3, :]
    curvature = jnp.where(own_ref[CORE] == 0, mine + other, other + mine)
    row = lax.broadcasted_iota(jnp.int32, tail_ref.shape, 0)
    tail = jnp.where(row == own_ref[DEPTH], curvature, 0.0)
    tail_ref[...] = tail
    rhs = two_parts(weighted)
    rhs_ref[...] = rhs
    part = parts_ref.shape[1] // 2
    add_product(parts_ref, side, rhs, base_ref, (1 - own_ref[LEAD]) * part, send_ref, part)
    send_ref[part:, :] = tail


def exchange_keep(own_ref, parts_ref, base_ref, rhs_ref, tail_ref, keep_ref):
    part = parts_ref.shape[1] // 2
    side = 1 - own_ref[CORE]
    add_product(parts_ref, side, rhs_ref[...], base_ref, own_ref[LEAD] * part, keep_ref, part)
    keep_ref[part:, :] = tail_ref[...]


def finish_own(own_ref, energy_ref, fixed_ref, y_ref, r_ref, v_ref, next_ref, square_ref, alpha_ref):
    r, _, alpha_ref[...] = advance_own(own_ref, energy_ref, fixed_ref, y_ref, r_ref, v_ref)
    next_ref[...] = r
    square_ref[...] = block_of([column_sum(r * r)])


def finish_other(own_ref, energy_ref, fixed_ref, alpha_ref, y_ref, r_ref, v_ref, own_half_ref, out_ref):
    side = own_ref[LEAD]
    part = own_half_ref.shape[0]
    other, _ = advance_other(own_ref, energy_ref, fixed_ref, alpha_ref, y_ref, r_ref, v_ref)
    out_ref[pl.ds(pl.multiple_of(side * part, ROWS), part), :] = own_half_ref[...]
    out_ref[pl.ds(pl.multiple_of((1 - side) * part, ROWS), part), :] = other


def swaps(size, bit):
    return [(i, i ^ bit) for i in range(size)]


def bits_of(size):
    return [1 << b for b in range(size.bit_length() - 1)]


def crossed_swaps(size):
    bits = bits_of(size)[1:]
    turned = bits[::-1]
    return [
        [(i, i ^ (turned[n] if i & 1 else bits[n])) for i in range(size)] for n in range(len(bits))
    ]


def depth_swaps(ka, ga):
    bits = bits_of(ga)
    orders = [bits, bits[1:2] + bits[:1] + bits[2:]]
    return [
        [(a * ga + g, a * ga + (g ^ orders[a & 1][n])) for a in range(ka) for g in range(ga)]
        for n in range(len(bits))
    ]


def chunks(size, cuts):
    edges = [0] + [size * c // 16 // ROWS * ROWS for c in cuts] + [None]
    return [slice(*pair) for pair in zip(edges[:-1], edges[1:])][::-1]


def size_of(at, size):
    return (size if at.stop is None else at.stop) - at.start


def joined(pieces):
    return [jnp.concatenate(part, axis=0) for part in zip(*pieces)]


def per_device(ka, ga, pair_densities, energies, coulomb, start):
    rows, cols = pair_densities.shape
    half_r, half_g = rows // 2, cols // 2
    chips = ka // 2
    s_rows = -(-2 * chips // ROWS) * ROWS
    z_rows = -(-ga // ROWS) * ROWS
    core, chip, depth = lax.axis_index("ka") & 1, lax.axis_index("ka") >> 1, lax.axis_index("ga")
    lead = jnp.where(core == 0, depth & 1, (depth >> 1) & 1)
    own = jnp.stack([core, lead, depth, chip]).astype(jnp.int32)
    parts, t_parts = pl.pallas_call(
        split_matrix,
        out_shape=[
            jax.ShapeDtypeStruct((2, rows, cols), B16),
            jax.ShapeDtypeStruct((2, cols, rows), B16),
        ],
        in_specs=[SMEM, pl.BlockSpec(memory_space=pltpu.HBM)],
        out_specs=[VMEM] * 2,
        scratch_shapes=[
            pltpu.VMEM((rows, cols), F32),
            pltpu.SemaphoreType.DMA((rows // min(half_r, 128),)),
        ],
        cost_estimate=pl.CostEstimate(flops=2**31, bytes_accessed=0, transcendentals=0),
        compiler_params=pltpu.CompilerParams(vmem_limit_bytes=34 * MIB),
    )(own, pair_densities)
    energy = jnp.broadcast_to(energies[:, None], (rows, LANES))
    weights = jnp.broadcast_to(coulomb[:, None], (cols, LANES))

    flops = rows * cols * LANES * 4
    edge = half_g * KA_CUT // 16 // LANES * LANES or LANES
    line, block, half = ((1, LANES), F32), ((ROWS, LANES), F32), ((half_r, LANES), F32)
    wide = 2 * LANES
    both = ("ka", "ga")
    first_round, *rounds = depth_swaps(ka, ga)

    alphas, betas = [], []
    r = v = fixed = y_own = y_other = None
    for step in range(ITERS):
        outs = [((half_g + s_rows, LANES), F32), ((half_r, wide), B16), ((s_rows, LANES), F32)]
        if step == 0:
            outs[1] = ((2, half_r, wide), B16)
            send, rhs, tail, *r = call(
                functools.partial(first_send, chips=chips),
                outs + [half, half],
                flops // 2,
                own,
                t_parts,
                energy,
                start,
            )
            v = (jnp.zeros_like(r[0]),) * 2
        else:
            base, sums, r_own, v_own, alpha = call(
                project_own,
                [((cols, LANES), F32), block, half, half, line],
                flops // 2,
                own,
                t_parts,
                energy,
                fixed,
                y_own,
                r[0],
                v[0],
            )
            send, rhs, tail, r_other, v_other = call(
                functools.partial(project_send, chips=chips),
                outs + [half, half],
                flops // 4,
                own,
                t_parts,
                energy,
                base,
                sums,
                fixed,
                alpha,
                y_other,
                r[1],
                v[1],
            )
            r, v = (r_own, r_other), (v_own, v_other)
            alphas.append(alpha)
        arrived = lax.ppermute(send, "ka", swaps(ka, 1))
        if step == 0:
            (keep,) = call(first_keep, outs[:1], flops // 2, own, t_parts, rhs, tail)
        else:
            (keep,) = call(project_keep, outs[:1], flops // 4, own, t_parts, base, rhs, tail)
        pieces = []
        for at in (slice(edge, None), slice(0, edge)):
            held = keep[at] + arrived[at]
            for pairs in crossed_swaps(ka):
                came = lax.ppermute(held, "ka", pairs)
                held = held + came
            pieces.insert(0, (held, lax.ppermute(held[: size_of(at, half_g)], "ka", swaps(ka, 1))))
        (held, head), (_, other) = pieces[1][:1] + pieces[0][:1], joined(pieces)
        base, fixed = call(
            functools.partial(exchange_first, chips=chips, edge=edge),
            [((rows, LANES), F32), block],
            flops // 4,
            own,
            parts,
            weights,
            held,
        )
        base, fixed = call(
            exchange_more, [((rows, LANES), F32), block], flops // 4, own, parts, weights, head, base, fixed
        )
        if step > 0:
            betas.append(fixed[0:1])
        outs = [((half_r + z_rows, LANES), F32), ((half_g, wide), B16), ((z_rows, LANES), F32)]
        send, rhs, tail = call(
            functools.partial(exchange_send, edge=edge), outs, flops // 4, own, parts, weights, base, fixed, other
        )
        pieces = []
        arrived = [
            lax.ppermute(send[at], both, first_round) for at in chunks(half_r, GA_CUTS)
        ]
        (keep,) = call(exchange_keep, outs[:1], flops // 4, own, parts, base, rhs, tail)
        for at, part in zip(chunks(half_r, GA_CUTS), arrived):
            y_own = keep[at] + part
            for pairs in rounds:
                y_own = y_own + lax.ppermute(y_own, both, pairs)
            y_part = y_own[: size_of(at, half_r)]
            y_part = lax.ppermute(y_part, both, first_round)
            pieces.insert(0, (y_own, y_part))
        y_own, y_other = joined(pieces)
    r_own, square, alpha = call(finish_own, [half, block, line], 2**20, own, energy, fixed, y_own, r[0], v[0])
    alphas.append(alpha)
    came = lax.ppermute(square, both, first_round)
    square = square + came
    for bit in bits_of(ka):
        came = lax.ppermute(square, "ka", swaps(ka, bit))
        square = square + came
    (last,) = call(
        finish_other,
        [((rows, LANES), F32)],
        flops // 4,
        own,
        energy,
        fixed,
        alpha,
        y_other,
        r[1],
        v[1],
        r_own,
    )
    beta = jnp.sqrt(square[0:1] + EPSILON)
    betas.append(beta)
    return (
        jnp.concatenate(alphas, axis=0),
        jnp.concatenate(betas, axis=0),
        last / beta,
    )


def solution(mesh):
    placed = (P("ka", "ga"), P("ka"), P("ga"), P("ka", None))
    return jax.shard_map(
        functools.partial(per_device, mesh.shape["ka"], mesh.shape["ga"]),
        mesh=mesh,
        in_specs=placed,
        out_specs=(P(), P(), P("ka", None)),
        check_vma=False,
    )
```
